32 devices in a mesh: groups: 2 (over x), mp: 16 (over z, y, core).
Axes of the slice: x: 2, y: 2, z: 4, core: 2. Of those that a mesh axis runs over, the one named last changes fastest.
Arguments:
- hidden: bfloat16 [1024, 4096], P(('groups', 'mp')), parts along dimension 0, may hold values from -6 to 6
- norm_gain_attn: float32 [4096], replicated, may hold values from 0.5 to 1.5
- w_query: bfloat16 [4096, 1024], P(None, 'mp'), may hold values from -0.09375 to 0.09375
- entering_kv: bfloat16 [16, 2048, 2048], P('groups', 'mp'), parts along dimension 0, may hold values from -60 to 60
- cached_kv: bfloat16 [16, 2048, 2048], P('groups', None, 'mp'), parts along dimension 0, may hold values from -60 to 60
- enc_lengths: int32 [2, 16], P(None, 'groups'), parts along dimension 1, may hold values from 128 to 2048
- w_out: bfloat16 [1024, 4096], P('mp'), may hold values from -0.1875 to 0.1875
- norm_gain_ffn: float32 [4096], replicated, may hold values from 0.5 to 1.5
- w_gate: bfloat16 [4096, 10240], P(None, 'mp'), may hold values from -0.09375 to 0.09375
- w_up: bfloat16 [4096, 10240], P(None, 'mp'), may hold values from -0.09375 to 0.09375
- w_down: bfloat16 [10240, 4096], P('mp'), may hold values from -0.0625 to 0.0625
Outputs:
- output: bfloat16 [1024, 4096], P(('groups', 'mp')), parts along dimension 0
The draws below stay inside these ranges and needn't reach their ends.
There are 2 independent parts, one for each index of `groups`. The reference program is written for one: setup_inputs(seed, part) draws one part's arguments, and reference() takes and returns one part's arrays. A program takes and returns all parts, laid end to end along the dimension named above; an argument that names none is the same for every part. Nothing has to cross between parts.
All inputs are finite; a program needn't handle non-finite values.
Results may differ from the reference program's by a relative error of at most 0.0095.
The reference program's roundings to bfloat16 on the way (of `normed_in`, `query`, `weights`, `context`, `residual`, `normed_ffn` and `activated`) count: a program that leaves them out, or rounds other values in their place, can miss the bound.
Values may be sent and summed in bfloat16 or wider, within the bound.
A program may use at most 128 MiB of HBM per device.

```python
import jax
import jax.numpy as jnp
from jax import lax

D = 4096
DH = 64
FF = 10240
H = 16
S = 2048
QLEN = 32
REQ = 8
TOK = 512


def kv_block(seed_key):
    width = 2 * H * DH
    base = jnp.clip(jax.random.normal(seed_key, (REQ, S, width), jnp.float32), -4.5, 4.5)
    return base.astype(jnp.bfloat16)


def draw_entering_kv(key, part):
    return kv_block(jax.random.fold_in(key, 11))


def draw_cached_kv(key, part):
    return kv_block(jax.random.fold_in(key, 23))


def place_ends(result, stream_key, smallest, top_value):
    longest = result.shape.index(max(result.shape))
    spots = []
    for shift in (0, 1):
        where = [jax.random.randint(jax.random.fold_in(stream_key, axis), (), 0, length) for axis, length in enumerate(result.shape)]
        where[longest] = (where[longest] + shift) % result.shape[longest]
        spots.append(tuple(where))
    return result.at[spots[0]].set(smallest).at[spots[1]].set(top_value)


def steps_of(own_key, extent, split, least, high):
    def one(dim, blocks):
        heights = jax.random.uniform(jax.random.fold_in(jax.random.fold_in(own_key, 6), dim), (blocks,), jnp.float32, least / len(split), high / len(split))
        return jnp.repeat(jnp.exp(heights), extent[dim] // blocks).reshape((-1,) + (1,) * (len(extent) - dim - 1))

    factor_of = one(*split[0])
    for cut in split[1:]:
        factor_of = factor_of * one(*cut)
    return factor_of


def gaussian(own_key, extent, scale, limit, pieces=(), kind=jnp.bfloat16):
    entries = jax.random.normal(own_key, extent, jnp.float32) * scale
    if len(pieces) > 0:
        entries = steps_of(own_key, extent, pieces, -0.22, 0.18) * entries
    return jnp.clip(entries, min=-limit, max=limit).astype(kind)


def setup_inputs(seed: int = 0, part: int = 0) -> dict:
    key_of = jax.random.split(jax.random.key(seed), 12)
    part_keys = jax.random.split(jax.random.fold_in(key_of[11], part), 12)
    hidden = gaussian(part_keys[0], (TOK, D), 1.0, 6.0, ((0, 16),))
    norm_gain_attn = jnp.clip(1.0 + 0.1 * jax.random.normal(key_of[1], (D,), jnp.float32), 0.5, 1.5)
    w_query = gaussian(key_of[2], (D, H * DH), D ** -0.5, 0.09375, ((1, 16),))
    entering_kv = draw_entering_kv(jax.random.fold_in(jax.random.fold_in(key_of[11], part), 71), part)
    cached_kv = draw_cached_kv(jax.random.fold_in(jax.random.fold_in(key_of[11], part), 71), part)
    enc_lengths = place_ends(jax.random.randint(part_keys[5], (2, REQ), S // 16, S + 1), jax.random.fold_in(part_keys[5], 1), S // 16, S).astype(jnp.int32)
    w_out = gaussian(key_of[6], (H * DH, D), (H * DH) ** -0.5, 0.1875, ((0, 16),))
    norm_gain_ffn = jnp.clip(1.0 + 0.1 * jax.random.normal(key_of[7], (D,), jnp.float32), 0.5, 1.5)
    w_gate = gaussian(key_of[8], (D, FF), D ** -0.5, 0.09375, ((1, 16),))
    w_up = gaussian(key_of[9], (D, FF), D ** -0.5, 0.09375, ((1, 16),))
    w_down = gaussian(key_of[10], (FF, D), FF ** -0.5, 0.0625, ((0, 16),))
    return {"hidden": hidden, "norm_gain_attn": norm_gain_attn, "w_query": w_query, "entering_kv": entering_kv, "cached_kv": cached_kv, "enc_lengths": enc_lengths, "w_out": w_out, "norm_gain_ffn": norm_gain_ffn, "w_gate": w_gate, "w_up": w_up, "w_down": w_down}


epsilon = 0.1

def normalize(matrix, gain_row):
    values = matrix.astype(jnp.float32)
    mean_square = lax.optimization_barrier(jnp.mean(values * values, axis=-1, keepdims=True))
    return (values * lax.rsqrt(mean_square + epsilon) * gain_row).astype(jnp.bfloat16)

def attend(query, key_value, lengths):
    requests = lengths.shape[0]
    head_count = key_value.shape[2] // (2 * DH)
    query_heads = query.reshape(requests, QLEN, head_count, DH).astype(jnp.float32)
    paired = key_value.reshape(requests, S, head_count, 2, DH).astype(jnp.float32)
    key_part = paired[:, :, :, 0, :]
    value_part = paired[:, :, :, 1, :]
    scores = jnp.einsum('rqhd,rshd->rhqs', query_heads, key_part)
    usable = (jnp.arange(S, dtype=jnp.int32)[None, :] < lengths[:, None].astype(jnp.int32))[:, None, None, :]
    masked = jnp.where(usable, scores, -1e+30)
    largest = lax.optimization_barrier(jnp.max(masked, axis=-1, keepdims=True))
    exponent = jnp.where(usable, jnp.exp(masked - largest), 0.0)
    weights = (exponent / lax.optimization_barrier(jnp.sum(exponent, axis=-1, keepdims=True))).astype(jnp.bfloat16)
    context = jnp.einsum('rhqs,rshd->rqhd', weights.astype(jnp.float32), value_part)
    return context.astype(jnp.bfloat16).reshape(requests * QLEN, head_count * DH)

def reference(hidden, norm_gain_attn, w_query, entering_kv, cached_kv, enc_lengths, w_out, norm_gain_ffn, w_gate, w_up, w_down):
    normed_in = normalize(hidden, norm_gain_attn)
    query = jnp.dot(normed_in, w_query, preferred_element_type=jnp.float32).astype(jnp.bfloat16)
    split_row = REQ * QLEN
    context = jnp.concatenate([attend(query[:split_row], entering_kv, enc_lengths[0]), attend(query[split_row:], cached_kv, enc_lengths[1])], axis=0)
    attention = jnp.dot(context, w_out, preferred_element_type=jnp.float32)
    residual = (hidden.astype(jnp.float32) + attention).astype(jnp.bfloat16)
    normed_ffn = normalize(residual, norm_gain_ffn)
    gate = jnp.dot(normed_ffn, w_gate, preferred_element_type=jnp.float32)
    upward = jnp.dot(normed_ffn, w_up, preferred_element_type=jnp.float32)
    activated = (jax.nn.gelu(gate, approximate=True) * upward).astype(jnp.bfloat16)
    return (residual.astype(jnp.float32) + jnp.dot(activated, w_down, preferred_element_type=jnp.float32)).astype(jnp.bfloat16)
```

```python
import functools

import jax
import jax.numpy as jnp
from jax import lax
from jax.experimental import pallas as pl
from jax.experimental.pallas import tpu as pltpu
from jax.sharding import PartitionSpec as P

DH = 64
QLEN = 32
PAD = 2 * DH
MESH = pl.DeviceIdType.MESH
VM = pltpu.VMEM
DMA = pltpu.SemaphoreType.DMA

epsilon = 0.1


def normalize(matrix, gain_row):
    values = matrix.astype(jnp.float32)
    mean_square = jnp.mean(values * values, axis=-1, keepdims=True)
    return (values * lax.rsqrt(mean_square + epsilon) * gain_row).astype(jnp.bfloat16)


def place(n):
    me = lax.axis_index("mp")
    return me, me // 4, (me // 2) % 2, me % 2


def index_of(a, b, c):
    return (a * 2 + b) * 2 + c


def remote(src, dst, send, recv, to):
    return pltpu.make_async_remote_copy(
        src_ref=src, dst_ref=dst, send_sem=send, recv_sem=recv, device_id={"mp": to}, device_id_type=MESH
    )


def greet(to):
    pl.semaphore_signal(pltpu.get_barrier_semaphore(), inc=1, device_id={"mp": to}, device_id_type=MESH)


def gather_kernel(n, x_ref, out_ref, zs, zr, ys, yr, cs, cr):
    A = n // 4
    me, a, b, c = place(n)
    across, pair = index_of(a, 1 - b, c), index_of(a, b, 1 - c)
    right, left = me + 4, me - 4
    has = {1: a < A - 1, -1: a > 0}
    toward = {1: right, -1: left}
    for d in (1, -1):

        @pl.when(has[d])
        def _():
            greet(toward[d])

    greet(across)
    greet(pair)
    pl.semaphore_wait(
        pltpu.get_barrier_semaphore(), 2 + has[1].astype(jnp.int32) + has[-1].astype(jnp.int32)
    )

    def z_copy(src, k, s, d):
        row = 0 if d == 1 else A
        return remote(src, out_ref.at[index_of(k, b, c)], zs.at[row + s], zr.at[k], toward[d])

    def y_copy(src, k, bb):
        return remote(src, out_ref.at[index_of(k, bb, c)], ys.at[k], yr.at[k], across)

    def c_copy(src, k, bb, cc):
        return remote(src, out_ref.at[index_of(k, bb, cc)], cs.at[bb * A + k], cr.at[bb * A + k], pair)

    for d in (1, -1):

        @pl.when(has[d])
        def _():
            z_copy(x_ref, a, 0, d).start()

    y_copy(x_ref, a, b).start()
    c_copy(x_ref, a, b, c).start()
    out_ref[me] = x_ref[...]

    def pass_on(s):
        for d in (1, -1) if s else (1,):
            k = a - s * d

            @pl.when((k >= 0) & (k < A))
            def _():
                y_copy(x_ref, k, 1 - b).wait_recv()
                c_copy(out_ref.at[index_of(k, 1 - b, c)], k, 1 - b, c).start()

    for s in range(1, A):
        for d in (1, -1):
            k = a - s * d

            @pl.when((k >= 0) & (k < A))
            def _():
                block = out_ref.at[index_of(k, b, c)]
                remote(x_ref, block, zs.at[0], zr.at[k], toward[-d]).wait_recv()

                @pl.when(has[d])
                def _():
                    z_copy(block, k, s, d).start()

                y_copy(block, k, b).start()
                c_copy(block, k, b, c).start()

        pass_on(s - 1)
    pass_on(A - 1)
    for bb in range(2):
        for k in range(A):
            c_copy(x_ref, k, bb, 1 - c).wait_recv()
    for s in range(A):
        for d in (1, -1):
            k = a - s * d

            @pl.when((k >= 0) & (k < A) & has[d])
            def _():
                z_copy(x_ref, k, s, d).wait_send()

    for k in range(A):
        y_copy(x_ref, k, b).wait_send()
        for bb in range(2):
            c_copy(x_ref, k, bb, c).wait_send()


def params(number):
    return pltpu.CompilerParams(collective_id=number, has_side_effects=True, vmem_limit_bytes=56 * 2**20)


def gather(x, n, number):
    A = n // 4
    return pl.pallas_call(
        functools.partial(gather_kernel, n),
        out_shape=jax.ShapeDtypeStruct((n,) + x.shape, x.dtype),
        in_specs=[pl.BlockSpec(memory_space=VM)],
        out_specs=pl.BlockSpec(memory_space=VM),
        scratch_shapes=[DMA((2 * A,)), DMA((A,)), DMA((A,)), DMA((A,)), DMA((2 * A,)), DMA((2 * A,))],
        compiler_params=params(number),
        name=f"gather_{number}",
    )(x)


def scatter_kernel(n, part_ref, out_ref, cbuf, ysend, yrecv, zsend, zrecv, cs, cr, ys, yr, zs, zr):
    A = n // 4
    me, a, b, c = place(n)
    across, pair = index_of(a, 1 - b, c), index_of(a, b, 1 - c)
    order = sorted(range(A), key=lambda s: -min(s, A - s))
    for s in range(1, A):
        greet(index_of(lax.rem(a + s, A), b, c))
    greet(across)
    greet(pair)
    pl.semaphore_wait(pltpu.get_barrier_semaphore(), A + 1)

    def c_copy(k, bb, cc):
        slot = bb * A + k
        return remote(part_ref.at[index_of(k, bb, cc)], cbuf.at[slot], cs.at[slot], cr.at[slot], pair)

    def y_copy(k):
        return remote(ysend.at[k], yrecv.at[k], ys.at[k], yr.at[k], across)

    def z_copy(k):
        return remote(zsend.at[k], zrecv.at[a], zs.at[k], zr.at[a], index_of(k, b, c))

    ks = [lax.rem(a + s, A) for s in order]
    for bb in (1 - b, b):
        for k in ks:
            c_copy(k, bb, 1 - c).start()
    for k in ks:
        c_copy(k, 1 - b, 1 - c).wait_recv()
        total = part_ref[index_of(k, 1 - b, c)] + cbuf[(1 - b) * A + k]
        ysend[k] = total.astype(jnp.bfloat16)
        y_copy(k).start()
    for s, k in zip(order, ks):
        c_copy(k, b, 1 - c).wait_recv()
        y_copy(k).wait_recv()
        total = part_ref[index_of(k, b, c)] + cbuf[b * A + k] + yrecv[k].astype(jnp.float32)
        if s:
            zsend[k] = total.astype(jnp.bfloat16)
            z_copy(k).start()
        else:
            out_ref[...] = total
    for s, k in zip(order, ks):
        if s:
            remote(zsend.at[k], zrecv.at[k], zs.at[k], zr.at[k], index_of(k, b, c)).wait_recv()
            out_ref[...] += zrecv[k].astype(jnp.float32)
    for s, k in zip(order, ks):
        y_copy(k).wait_send()
        if s:
            z_copy(k).wait_send()
        for bb in range(2):
            c_copy(k, bb, 1 - c).wait_send()


def scatter(part, n, number):
    A = n // 4
    block = (part.shape[0] // n, part.shape[1])
    half = jnp.bfloat16
    return pl.pallas_call(
        functools.partial(scatter_kernel, n),
        out_shape=jax.ShapeDtypeStruct(block, jnp.float32),
        in_specs=[pl.BlockSpec(memory_space=VM)],
        out_specs=pl.BlockSpec(memory_space=VM),
        scratch_shapes=[VM((2 * A,) + block, jnp.float32)]
        + [VM((A,) + block, half)] * 4
        + [DMA((2 * A,)), DMA((2 * A,)), DMA((A,)), DMA((A,)), DMA((A,)), DMA((A,))],
        compiler_params=params(number),
        name=f"scatter_{number}",
    )(part.reshape((n,) + block))


def exchange_kernel(n, o_ref, st_ref, o_out, st_out, s0, r0, s1, r1):
    me = lax.axis_index("mp")
    for s in range(1, n):
        greet(lax.rem(me + s, n))
    pl.semaphore_wait(pltpu.get_barrier_semaphore(), n - 1)

    def copies(s, mine):
        other = lax.rem(me + s, n)
        spot = me if mine else other
        return (
            remote(o_ref.at[other], o_out.at[spot], s0.at[other], r0.at[spot], other),
            remote(st_ref.at[other], st_out.at[spot], s1.at[other], r1.at[spot], other),
        )

    order = sorted(range(1, n), key=lambda s: -min(s, n - s))
    for s in order:
        for copy in copies(s, True):
            copy.start()
    o_out[me] = o_ref[me]
    st_out[me] = st_ref[me]
    for s in order:
        for copy in copies(s, False):
            copy.wait_recv()
    for s in order:
        for copy in copies(s, True):
            copy.wait_send()


def exchange(o, st, n, number):
    return pl.pallas_call(
        functools.partial(exchange_kernel, n),
        out_shape=(jax.ShapeDtypeStruct(o.shape, o.dtype), jax.ShapeDtypeStruct(st.shape, st.dtype)),
        in_specs=[pl.BlockSpec(memory_space=VM)] * 2,
        out_specs=[pl.BlockSpec(memory_space=VM)] * 2,
        scratch_shapes=[DMA((n,))] * 4,
        compiler_params=params(number),
        name=f"exchange_{number}",
    )(o, st)


def pieces_kernel(heads, q_ref, kv_ref, mask_ref, o_ref, st_ref):
    step = pl.program_id(0)
    lane = lax.broadcasted_iota(jnp.int32, (QLEN, PAD), 1)

    @pl.when(step == 0)
    def _():
        st_ref[...] = jnp.zeros_like(st_ref)

    for h in range(heads):
        found = []
        stats = st_ref[h]
        for i in range(2):
            block = kv_ref[i, :, h * PAD : (h + 1) * PAD]
            scores = lax.dot_general(
                q_ref[h, i * QLEN : (i + 1) * QLEN, :], block, (((1,), (1,)), ((), ())),
                preferred_element_type=jnp.float32,
            )
            usable = mask_ref[i] > 0.5
            masked = jnp.where(usable, scores, -1e30)
            largest = jnp.max(masked, axis=-1, keepdims=True)
            exponent = jnp.where(usable, jnp.exp(masked - largest), 0.0)
            total = jnp.sum(exponent, axis=-1, keepdims=True)
            r = step * 2 + i
            stats = jnp.where(lane == r, largest, jnp.where(lane == r + DH, total, stats))
            found.append(jnp.dot(exponent.astype(jnp.bfloat16), block, preferred_element_type=jnp.float32))
        st_ref[h] = stats
        o_ref[h] = jnp.where(lane < DH, pltpu.roll(found[1], DH, 1), found[0]).astype(jnp.bfloat16)


def attend_pieces(query, key_value, lengths, n):
    requests, positions, width = key_value.shape
    heads = width // PAD
    start = lax.axis_index("mp") * positions
    usable = (start + jnp.arange(positions, dtype=jnp.int32))[None, :] < lengths[:, None]
    mask = usable.astype(jnp.float32)[:, None, :]
    o, st = pl.pallas_call(
        functools.partial(pieces_kernel, heads),
        grid=(requests // 2,),
        out_shape=(
            jax.ShapeDtypeStruct((heads, requests // 2 * QLEN, PAD), jnp.bfloat16),
            jax.ShapeDtypeStruct((heads, QLEN, PAD), jnp.float32),
        ),
        in_specs=[
            pl.BlockSpec((heads, 2 * QLEN, PAD), lambda r: (0, r, 0)),
            pl.BlockSpec((2, positions, width), lambda r: (r, 0, 0)),
            pl.BlockSpec((2, 1, positions), lambda r: (r, 0, 0)),
        ],
        out_specs=[
            pl.BlockSpec((heads, QLEN, PAD), lambda r: (0, r, 0)),
            pl.BlockSpec((heads, QLEN, PAD), lambda r: (0, 0, 0)),
        ],
        name="pieces",
    )(query, key_value, mask)
    o, st = exchange(o, st, n, 2)
    largest, total = st[:, :, :requests], st[:, :, DH : DH + requests]
    scale = jnp.exp(largest - jnp.max(largest, axis=0, keepdims=True))
    share = scale / jnp.sum(scale * total, axis=0, keepdims=True)
    share = share.transpose(0, 2, 1).reshape(n, requests // 2, 2, QLEN, 1)
    o = o.astype(jnp.float32).reshape(n, requests // 2, QLEN, PAD)
    even = jnp.sum(share[:, :, 0] * o[..., DH:], axis=0)
    odd = jnp.sum(share[:, :, 1] * o[..., :DH], axis=0)
    return jnp.stack([even, odd], axis=1).reshape(requests * QLEN, DH).astype(jnp.bfloat16)


def attend(query, key_value, lengths):
    requests, positions, _ = key_value.shape
    query = query.reshape(requests, QLEN, PAD)
    scores = jnp.einsum("rqd,rsd->rqs", query, key_value, preferred_element_type=jnp.float32)
    usable = (jnp.arange(positions, dtype=jnp.int32)[None, :] < lengths[:, None])[:, None, :]
    masked = jnp.where(usable, scores, -1e30)
    largest = jnp.max(masked, axis=-1, keepdims=True)
    exponent = jnp.where(usable, jnp.exp(masked - largest), 0.0)
    weights = (exponent / jnp.sum(exponent, axis=-1, keepdims=True)).astype(jnp.bfloat16)
    context = jnp.einsum("rqs,rsd->rqd", weights, key_value, preferred_element_type=jnp.float32)
    return context[..., DH:].astype(jnp.bfloat16).reshape(requests * QLEN, DH)


def per_device(
    n,
    hidden,
    norm_gain_attn,
    w_query,
    entering_kv,
    cached_kv,
    enc_lengths,
    w_out,
    norm_gain_ffn,
    w_gate,
    w_up,
    w_down,
):
    width = hidden.shape[1]
    portion = gather(normalize(hidden, norm_gain_attn), n, 0).reshape(-1, width)
    query = jnp.dot(portion, w_query, preferred_element_type=jnp.float32).astype(jnp.bfloat16)
    query = jnp.pad(query, ((0, 0), (0, DH)))
    split_row = query.shape[0] // 2
    all_heads = gather(query[:split_row], n, 1)
    context = jnp.concatenate(
        [
            attend_pieces(all_heads, entering_kv, enc_lengths[0], n),
            attend(query[split_row:], cached_kv, enc_lengths[1]),
        ],
        axis=0,
    )
    attention = scatter(jnp.dot(context, w_out, preferred_element_type=jnp.float32), n, 3)
    residual = (hidden.astype(jnp.float32) + attention).astype(jnp.bfloat16)
    portion = gather(normalize(residual, norm_gain_ffn), n, 4).reshape(-1, width)
    gate = jnp.dot(portion, w_gate, preferred_element_type=jnp.float32)
    upward = jnp.dot(portion, w_up, preferred_element_type=jnp.float32)
    activated = (jax.nn.gelu(gate, approximate=True) * upward).astype(jnp.bfloat16)
    feed_out = scatter(jnp.dot(activated, w_down, preferred_element_type=jnp.float32), n, 5)
    return (residual.astype(jnp.float32) + feed_out).astype(jnp.bfloat16)


def solution(mesh):
    placed = (
        P(("groups", "mp"), None),
        P(),
        P(None, "mp"),
        P("groups", "mp", None),
        P("groups", None, "mp"),
        P(None, "groups"),
        P("mp", None),
        P(),
        P(None, "mp"),
        P(None, "mp"),
        P("mp", None),
    )
    return jax.shard_map(
        functools.partial(per_device, mesh.shape["mp"]),
        mesh=mesh,
        in_specs=placed,
        out_specs=P(("groups", "mp"), None),
        check_vma=False,
    )
```

```python
import functools

import jax
import jax.numpy as jnp
from jax import lax
from jax.experimental import pallas as pl
from jax.experimental.pallas import tpu as pltpu
from jax.sharding import PartitionSpec as P

DH = 64
QLEN = 32
PAD = 2 * DH
MESH = pl.DeviceIdType.MESH
VM = pltpu.VMEM
DMA = pltpu.SemaphoreType.DMA

epsilon = 0.1


def normalize(matrix, gain_row):
    values = matrix.astype(jnp.float32)
    mean_square = jnp.mean(values * values, axis=-1, keepdims=True)
    return (values * lax.rsqrt(mean_square + epsilon) * gain_row).astype(jnp.bfloat16)


def place(n):
    me = lax.axis_index("mp")
    return me, me // 4, (me // 2) % 2, me % 2


def index_of(a, b, c):
    return (a * 2 + b) * 2 + c


def remote(src, dst, send, recv, to):
    return pltpu.make_async_remote_copy(
        src_ref=src, dst_ref=dst, send_sem=send, recv_sem=recv, device_id={"mp": to}, device_id_type=MESH
    )


def greet(to):
    pl.semaphore_signal(pltpu.get_barrier_semaphore(), inc=1, device_id={"mp": to}, device_id_type=MESH)


def gather_kernel(n, x_ref, out_ref, zs, zr, ys, yr, cs, cr):
    A = n // 4
    me, a, b, c = place(n)
    across, pair = index_of(a, 1 - b, c), index_of(a, b, 1 - c)
    right, left = me + 4, me - 4
    has = {1: a < A - 1, -1: a > 0}
    toward = {1: right, -1: left}
    for d in (1, -1):

        @pl.when(has[d])
        def _():
            greet(toward[d])

    greet(across)
    greet(pair)
    pl.semaphore_wait(
        pltpu.get_barrier_semaphore(), 2 + has[1].astype(jnp.int32) + has[-1].astype(jnp.int32)
    )

    def z_copy(src, k, s, d):
        row = 0 if d == 1 else A
        return remote(src, out_ref.at[index_of(k, b, c)], zs.at[row + s], zr.at[k], toward[d])

    def y_copy(src, k, bb):
        return remote(src, out_ref.at[index_of(k, bb, c)], ys.at[k], yr.at[k], across)

    def c_copy(src, k, bb, cc):
        return remote(src, out_ref.at[index_of(k, bb, cc)], cs.at[bb * A + k], cr.at[bb * A + k], pair)

    for d in (1, -1):

        @pl.when(has[d])
        def _():
            z_copy(x_ref, a, 0, d).start()

    y_copy(x_ref, a, b).start()
    c_copy(x_ref, a, b, c).start()
    out_ref[me] = x_ref[...]

    def pass_on(s):
        for d in (1, -1) if s else (1,):
            k = a - s * d

            @pl.when((k >= 0) & (k < A))
            def _():
                y_copy(x_ref, k, 1 - b).wait_recv()
                c_copy(out_ref.at[index_of(k, 1 - b, c)], k, 1 - b, c).start()

    for s in range(1, A):
        for d in (1, -1):
            k = a - s * d

            @pl.when((k >= 0) & (k < A))
            def _():
                block = out_ref.at[index_of(k, b, c)]
                remote(x_ref, block, zs.at[0], zr.at[k], toward[-d]).wait_recv()

                @pl.when(has[d])
                def _():
                    z_copy(block, k, s, d).start()

                y_copy(block, k, b).start()
                c_copy(block, k, b, c).start()

        pass_on(s - 1)
    pass_on(A - 1)
    for bb in range(2):
        for k in range(A):
            c_copy(x_ref, k, bb, 1 - c).wait_recv()
    for s in range(A):
        for d in (1, -1):
            k = a - s * d

            @pl.when((k >= 0) & (k < A) & has[d])
            def _():
                z_copy(x_ref, k, s, d).wait_send()

    for k in range(A):
        y_copy(x_ref, k, b).wait_send()
        for bb in range(2):
            c_copy(x_ref, k, bb, c).wait_send()


def params(number):
    return pltpu.CompilerParams(collective_id=number, has_side_effects=True, vmem_limit_bytes=56 * 2**20)


def gather(x, n, number):
    A = n // 4
    return pl.pallas_call(
        functools.partial(gather_kernel, n),
        out_shape=jax.ShapeDtypeStruct((n,) + x.shape, x.dtype),
        in_specs=[pl.BlockSpec(memory_space=VM)],
        out_specs=pl.BlockSpec(memory_space=VM),
        scratch_shapes=[DMA((2 * A,)), DMA((A,)), DMA((A,)), DMA((A,)), DMA((2 * A,)), DMA((2 * A,))],
        compiler_params=params(number),
        name=f"gather_{number}",
    )(x)


def scatter_kernel(
    n, left_ref, w_ref, out_ref, part, cbuf, ysend, yrecv, zsend, zright, zleft, cs, cr, ys, yr, zs, zr
):
    A = n // 4
    me, a, b, c = place(n)
    across, pair = index_of(a, 1 - b, c), index_of(a, b, 1 - c)
    has = {1: a < A - 1, -1: a > 0}
    toward = {1: me + 4, -1: me - 4}
    landing = {1: zright, -1: zleft}
    rows, width = out_ref.shape
    for d in (1, -1):

        @pl.when(has[d])
        def _():
            greet(toward[d])

    greet(across)
    greet(pair)
    pl.semaphore_wait(
        pltpu.get_barrier_semaphore(), 2 + has[1].astype(jnp.int32) + has[-1].astype(jnp.int32)
    )

    def near_last(visit):
        for s in range(A - 1, -1, -1):
            for d in (1, -1) if s else (1,):
                k = a + s * d

                @pl.when((k >= 0) & (k < A))
                def _():
                    visit(s, d, k)

    def multiply(group, bb, cc):
        left = jnp.concatenate([left_ref[index_of(k, bb, cc)] for k in range(A)], axis=0)
        tile = min(width, 1024)

        def columns(t, carry):
            at = pl.ds(pl.multiple_of(t * tile, tile), tile)
            found = jnp.dot(left, w_ref[:, at], preferred_element_type=jnp.float32)
            part[group, :, :, at] = found.reshape(A, rows, tile)
            return carry

        lax.fori_loop(0, width // tile, columns, 0)

    def c_copy(group, k, bb):
        slot = bb * A + k
        return remote(part.at[group, k], cbuf.at[slot], cs.at[slot], cr.at[slot], pair)

    def y_copy(k):
        return remote(ysend.at[k], yrecv.at[k], ys.at[k], yr.at[k], across)

    def z_copy(k, d):
        row = 0 if d == 1 else A
        return remote(zsend.at[k], landing[d].at[k], zs.at[k], zr.at[row + k], toward[d])

    def z_arrival(k, d):
        row = 0 if d == 1 else A
        return remote(zsend.at[k], landing[d].at[k], zs.at[k], zr.at[row + k], toward[-d])

    multiply(0, 1 - b, 1 - c)
    near_last(lambda s, d, k: c_copy(0, k, 1 - b).start())
    multiply(1, 1 - b, c)

    def send_across(s, d, k):
        c_copy(0, k, 1 - b).wait_recv()
        ysend[k] = (part[1, k] + cbuf[(1 - b) * A + k]).astype(jnp.bfloat16)
        y_copy(k).start()

    near_last(send_across)
    multiply(2, b, 1 - c)
    near_last(lambda s, d, k: c_copy(2, k, b).start())
    multiply(3, b, c)

    def pass_on(s, d, k):
        c_copy(2, k, b).wait_recv()
        y_copy(k).wait_recv()
        part[3, k] = part[3, k] + cbuf[b * A + k] + yrecv[k].astype(jnp.float32)
        for came in (d,) if s else (1, -1):

            @pl.when(has[-came])
            def _():
                z_arrival(k, came).wait_recv()
                part[3, k] = part[3, k] + landing[came][k].astype(jnp.float32)

        if s:
            zsend[k] = part[3, k].astype(jnp.bfloat16)
            z_copy(k, d).start()
        else:
            out_ref[...] = part[3, k]

    near_last(pass_on)

    def finish(s, d, k):
        y_copy(k).wait_send()
        if s:
            z_copy(k, d).wait_send()
        c_copy(0, k, 1 - b).wait_send()
        c_copy(2, k, b).wait_send()

    near_last(finish)


def scatter(left, w, n, number):
    A = n // 4
    rows, depth = left.shape[0] // n, left.shape[1]
    block = (rows, w.shape[1])
    half = jnp.bfloat16
    return pl.pallas_call(
        functools.partial(scatter_kernel, n),
        out_shape=jax.ShapeDtypeStruct(block, jnp.float32),
        in_specs=[pl.BlockSpec(memory_space=VM)] * 2,
        out_specs=pl.BlockSpec(memory_space=VM),
        scratch_shapes=[VM((4, A) + block, jnp.float32), VM((2 * A,) + block, jnp.float32)]
        + [VM((A,) + block, half)] * 5
        + [DMA((2 * A,)), DMA((2 * A,)), DMA((A,)), DMA((A,)), DMA((A,)), DMA((2 * A,))],
        compiler_params=params(number),
        name=f"scatter_{number}",
    )(left.reshape(n, rows, depth), w)


def attend_kernel(
    n, q_ref, own_ref, kv_ref, cached_ref, mask_ref, cached_mask_ref, out_ref,
    q_all, kv, cached, scores, chances, o_send, o_recv, st_send, st_recv, local, qs, qr, os, orr, ss, sr,
):
    me = lax.axis_index("mp")
    requests, positions, width = kv.shape
    pairs, heads = requests // 2, width // PAD
    load_cached = pltpu.make_async_copy(cached_ref, cached, local.at[0])
    load_kv = pltpu.make_async_copy(kv_ref, kv, local.at[1])
    load_cached.start()
    load_kv.start()
    order = sorted(range(1, n), key=lambda s: -min(s, n - s))
    others = [lax.rem(me + s, n) for s in order]
    for other in others:
        greet(other)
    pl.semaphore_wait(pltpu.get_barrier_semaphore(), n - 1)

    def q_copy(other, spot):
        return remote(q_ref, q_all.at[spot], qs.at[other], qr.at[spot], other)

    def o_copy(other, spot, step):
        rows = pl.ds(pl.multiple_of(step * QLEN, QLEN), QLEN)
        return remote(
            o_send.at[other, rows], o_recv.at[spot, rows], os.at[step, other], orr.at[step, spot], other
        )

    def st_copy(other, spot):
        return remote(st_send.at[other], st_recv.at[spot], ss.at[other], sr.at[spot], other)

    for other in others:
        q_copy(other, me).start()
    q_all[me] = q_ref[...]
    lane = lax.broadcasted_iota(jnp.int32, (QLEN, PAD), 1)
    load_cached.wait()

    def cached_request(r, carry):
        rows = pl.ds(pl.multiple_of(r * QLEN, QLEN), QLEN)
        block = cached[r]
        found = lax.dot_general(
            own_ref[rows, :], block, (((1,), (1,)), ((), ())), preferred_element_type=jnp.float32
        )
        usable = cached_mask_ref[r] > 0.5
        masked = jnp.where(usable, found, -1e30)
        exponent = jnp.where(usable, jnp.exp(masked - jnp.max(masked, axis=-1, keepdims=True)), 0.0)
        weights = (exponent / jnp.sum(exponent, axis=-1, keepdims=True)).astype(jnp.bfloat16)
        to = pl.ds(pl.multiple_of((requests + r) * QLEN, QLEN), QLEN)
        out_ref[to, :] = jnp.dot(weights, block, preferred_element_type=jnp.float32).astype(jnp.bfloat16)
        return carry

    lax.fori_loop(0, requests, cached_request, 0)
    st_send[...] = jnp.zeros_like(st_send)
    load_kv.wait()
    for other in others:
        q_copy(other, other).wait_recv()

    def pair_step(step, carry):
        rows = pl.ds(pl.multiple_of(step * QLEN, QLEN), QLEN)
        low = lane < DH
        nothing = jnp.zeros((QLEN, PAD), jnp.bfloat16)
        for i in range(2):
            for g in range(heads // 2):
                two = []
                for h in (2 * g, 2 * g + 1):
                    packed = q_all[h, rows, :].astype(jnp.float32)
                    packed = packed if i == 0 else pltpu.roll(packed, DH, 1)
                    two.append(jnp.where(low, packed, 0.0).astype(jnp.bfloat16))
                spread = jnp.concatenate(
                    [
                        jnp.concatenate([two[0], nothing], axis=1),
                        jnp.concatenate([nothing, two[1]], axis=1),
                    ],
                    axis=0,
                )
                scores[i, g] = lax.dot_general(
                    spread, kv[step * 2 + i, :, g * 2 * PAD : (g + 1) * 2 * PAD], (((1,), (1,)), ((), ())),
                    preferred_element_type=jnp.float32,
                )
        for i in range(2):
            r = step * 2 + i
            usable = mask_ref[r] > 0.5
            masked = jnp.where(usable, scores[i], -1e30)
            largest = jnp.max(masked, axis=-1, keepdims=True)
            exponent = jnp.where(usable, jnp.exp(masked - largest), 0.0)
            total = jnp.sum(exponent, axis=-1, keepdims=True)
            chances[i] = exponent.astype(jnp.bfloat16)
            st_send[...] = jnp.where(
                lane == r,
                largest.reshape(heads, QLEN, 1),
                jnp.where(lane == r + DH, total.reshape(heads, QLEN, 1), st_send[...]),
            )
        for g in range(heads // 2):
            found = [
                jnp.dot(
                    chances[i, g], kv[step * 2 + i, :, g * 2 * PAD : (g + 1) * 2 * PAD],
                    preferred_element_type=jnp.float32,
                )
                for i in range(2)
            ]
            for e in range(2):
                even, odd = (f[e * QLEN : (e + 1) * QLEN, e * PAD : (e + 1) * PAD] for f in found)
                o_send[2 * g + e, rows, :] = jnp.where(low, pltpu.roll(odd, DH, 1), even).astype(jnp.bfloat16)
        for other in others:
            o_copy(other, me, step).start()
        return carry

    lax.fori_loop(0, pairs, pair_step, 0)
    for other in others:
        st_copy(other, me).start()
    o_recv[me] = o_send[me]
    st_recv[me] = st_send[me]
    for other in others:
        st_copy(other, other).wait_recv()
    largest = st_recv[...]
    scale = jnp.exp(largest - jnp.max(largest, axis=0, keepdims=True))
    total = jnp.sum(
        scale * pltpu.roll(largest.reshape(n * QLEN, PAD), DH, 1).reshape(n, QLEN, PAD), axis=0, keepdims=True
    )
    st_recv[...] = scale / jnp.where(total > 0.0, total, 1.0)
    for step in range(pairs):
        for other in others:
            o_copy(other, other, step).wait_recv()
        mixed = jnp.zeros((QLEN, PAD), jnp.float32)
        for d in range(n):
            share = st_recv[d]
            share = jnp.where(
                lane < DH, share[:, 2 * step + 1 : 2 * step + 2], share[:, 2 * step : 2 * step + 1]
            )
            mixed = mixed + share * o_recv[d, step * QLEN : (step + 1) * QLEN, :].astype(jnp.float32)
        out_ref[2 * step * QLEN : (2 * step + 1) * QLEN, :] = mixed.astype(jnp.bfloat16)
        out_ref[(2 * step + 1) * QLEN : (2 * step + 2) * QLEN, :] = pltpu.roll(mixed, DH, 1).astype(jnp.bfloat16)
    for other in others:
        q_copy(other, me).wait_send()
        st_copy(other, me).wait_send()
        for step in range(pairs):
            o_copy(other, me, step).wait_send()


def attend(query, entering_kv, cached_kv, lengths, n, number):
    requests, positions, width = entering_kv.shape
    length = cached_kv.shape[1]
    pairs, heads = requests // 2, width // PAD
    half = query.shape[0] // 2
    packed = query[:half].reshape(pairs, 2, QLEN, DH)
    packed = jnp.concatenate([packed[:, 0], packed[:, 1]], axis=-1).reshape(pairs * QLEN, PAD)
    own = jnp.pad(query[half:], ((0, 0), (0, DH)))
    start = lax.axis_index("mp") * positions
    usable = (start + jnp.arange(positions, dtype=jnp.int32))[None, :] < lengths[0][:, None]
    cached_usable = jnp.arange(length, dtype=jnp.int32)[None, :] < lengths[1][:, None]
    half_type = jnp.bfloat16
    context = pl.pallas_call(
        functools.partial(attend_kernel, n),
        out_shape=jax.ShapeDtypeStruct((2 * requests * QLEN, PAD), half_type),
        in_specs=[pl.BlockSpec(memory_space=m) for m in (VM, VM, pl.ANY, pl.ANY, VM, VM)],
        out_specs=pl.BlockSpec(memory_space=VM),
        scratch_shapes=[
            VM((n,) + packed.shape, half_type),
            VM(entering_kv.shape, half_type),
            VM(cached_kv.shape, half_type),
            VM((2, heads // 2, 2 * QLEN, positions), jnp.float32),
            VM((2, heads // 2, 2 * QLEN, positions), half_type),
            VM((n, pairs * QLEN, PAD), half_type),
            VM((n, pairs * QLEN, PAD), half_type),
            VM((n, QLEN, PAD), jnp.float32),
            VM((n, QLEN, PAD), jnp.float32),
            DMA((2,)), DMA((n,)), DMA((n,)), DMA((pairs, n)), DMA((pairs, n)), DMA((n,)), DMA((n,)),
        ],
        compiler_params=params(number),
        name=f"attend_{number}",
    )(
        packed, own, entering_kv, cached_kv,
        usable.astype(jnp.float32)[:, None, :], cached_usable.astype(jnp.float32)[:, None, :],
    )
    return context[:, DH:]


def per_device(
    n,
    hidden,
    norm_gain_attn,
    w_query,
    entering_kv,
    cached_kv,
    enc_lengths,
    w_out,
    norm_gain_ffn,
    w_gate,
    w_up,
    w_down,
):
    width = hidden.shape[1]
    portion = gather(normalize(hidden, norm_gain_attn), n, 0).reshape(-1, width)
    query = jnp.dot(portion, w_query, preferred_element_type=jnp.float32).astype(jnp.bfloat16)
    context = attend(query, entering_kv, cached_kv, enc_lengths, n, 1)
    attention = scatter(context, w_out, n, 3)
    residual = (hidden.astype(jnp.float32) + attention).astype(jnp.bfloat16)
    portion = gather(normalize(residual, norm_gain_ffn), n, 4).reshape(-1, width)
    gate = jnp.dot(portion, w_gate, preferred_element_type=jnp.float32)
    upward = jnp.dot(portion, w_up, preferred_element_type=jnp.float32)
    activated = (jax.nn.gelu(gate, approximate=True) * upward).astype(jnp.bfloat16)
    feed_out = scatter(activated, w_down, n, 5)
    return (residual.astype(jnp.float32) + feed_out).astype(jnp.bfloat16)


def solution(mesh):
    placed = (
        P(("groups", "mp"), None),
        P(),
        P(None, "mp"),
        P("groups", "mp", None),
        P("groups", None, "mp"),
        P(None, "groups"),
        P("mp", None),
        P(),
        P(None, "mp"),
        P(None, "mp"),
        P("mp", None),
    )
    return jax.shard_map(
        functools.partial(per_device, mesh.shape["mp"]),
        mesh=mesh,
        in_specs=placed,
        out_specs=P(("groups", "mp"), None),
        check_vma=False,
    )
```
